32 devices in a mesh: wide: 8 (over y, x, core), narrow: 4 (over z).
Axes of the slice: x: 2, y: 2, z: 4, core: 2. Of those that a mesh axis runs over, the one named last changes fastest.
Arguments:
- first_state: float32 [2, 32768, 1024], P(None, ('wide', 'narrow')), may hold values from -100 to 100
- second_state: float32 [2, 32768, 1024], P(None, ('wide', 'narrow')), may hold values from -200 to 200
- place_first: int32 [32768], replicated, may hold values from 0 to 32767, as said below
- place_second: int32 [32768], replicated, may hold values from 0 to 32767, as said below
Outputs:
- aligned: float32 [2, 32768, 1024], P(None, ('wide', 'narrow'))
- intersection: float32 [2], replicated
- norms: float32 [2], replicated
The draws below stay inside these ranges and needn't reach their ends.
Inputs may be any that keep to these rules, and one draw needn't show every extreme that they name: Each of place_first and place_second maps a logical block index to a storage block index by a permutation of the index's bits. Every logical bit that selects a device (the high bits of a storage index above its position within a device) in one state's order selects a block within a device in the other's, so each device holds exactly 32 blocks of the second state that the first state's order places on any given device. `place_second`: drawn together with place_first under the rule stated there.
All inputs are finite; a program needn't handle non-finite values.
Results may differ from the reference program's by a relative error of at most 0.00002.
Values sent between devices are 32-bit elements; how exact they have to be, the bound alone decides.
No kernel may reach another device: no remote copies, remote signals or barrier semaphores. Data moves between devices by JAX's collectives and lax.ppermute only.
A program may use at most 128 MiB of HBM per device.

```python
import math
import jax
import jax.numpy as jnp
from jax import lax

BLOCK = 1024
BLOCKS_DEV = 1024
BLOCKS = 32768
AMPS = 33554432


def block_maps(key):
    block_bits = int(BLOCKS).bit_length() - 1
    global_bits = int(BLOCKS // BLOCKS_DEV).bit_length() - 1
    local_bits = block_bits - global_bits
    sigma = jax.random.permutation(jax.random.fold_in(key, 11), block_bits).astype(jnp.int32)
    device_first = sigma[:global_bits]
    device_second = sigma[global_bits:2 * global_bits]
    others = sigma[2 * global_bits:]
    order_first = jax.random.permutation(jax.random.fold_in(key, 12), local_bits).astype(jnp.int32)
    order_second = jax.random.permutation(jax.random.fold_in(key, 13), local_bits).astype(jnp.int32)
    local_first = jnp.concatenate([device_second, others])[order_first]
    local_second = jnp.concatenate([device_first, others])[order_second]
    map_first = jnp.concatenate([local_first, device_first]).astype(jnp.int32)
    map_second = jnp.concatenate([local_second, device_second]).astype(jnp.int32)
    return (map_first, map_second)


def storage_of(logical, bit_map):
    block_bits = int(BLOCKS).bit_length() - 1
    store = jnp.zeros_like(logical)
    for level in range(block_bits):
        store = store + jnp.left_shift(jnp.right_shift(logical, bit_map[level]) & 1, level)
    return store.astype(jnp.int32)


def logical_of(store, bit_map):
    block_bits = int(BLOCKS).bit_length() - 1
    logical = jnp.zeros_like(store)
    for level in range(block_bits):
        logical = logical + jnp.left_shift(jnp.right_shift(store, level) & 1, bit_map[level])
    return logical.astype(jnp.int32)


def block_scale(key, expo):
    steps = jnp.arange(BLOCKS, dtype=jnp.float32) / float(max(BLOCKS - 1, 1))
    rising = jnp.exp(expo * math.log(3.0) * steps)
    spread = jnp.exp(jax.random.uniform(key, (BLOCKS,), jnp.float32, 0.0, 0.5 * math.log(10.0)))
    return rising * spread


def base_normals(key):
    return jnp.clip(jax.random.normal(jax.random.fold_in(key, 31), (2, BLOCKS, BLOCK), jnp.float32), -6.0, 6.0)


def draw_place_first(key, part):
    map_first, map_second = block_maps(key)
    return storage_of(jnp.arange(BLOCKS, dtype=jnp.int32), map_first)


def draw_place_second(key, part):
    map_first, map_second = block_maps(key)
    return storage_of(jnp.arange(BLOCKS, dtype=jnp.int32), map_second)


def draw_first_state(key, part):
    expo = 0.5
    scale_first = block_scale(jax.random.fold_in(key, 21), expo)
    return base_normals(key) * scale_first[None, :, None]


def draw_second_state(key, part):
    expo = 0.5
    map_first, map_second = block_maps(key)
    logical = logical_of(jnp.arange(BLOCKS, dtype=jnp.int32), map_second)
    rows_first = storage_of(logical, map_first)
    shared = jnp.take(base_normals(key), rows_first, axis=1)
    angles = jax.random.uniform(jax.random.fold_in(key, 41), (BLOCKS,), jnp.float32, 0.3, 1.2)
    cosine = jnp.cos(angles)[:, None]
    sine = jnp.sin(angles)[:, None]
    turned = jnp.stack([cosine * shared[0] - sine * shared[1], sine * shared[0] + cosine * shared[1]])
    noise = jnp.clip(jax.random.normal(jax.random.fold_in(key, 32), (2, BLOCKS, BLOCK), jnp.float32), -6.0, 6.0)
    scale_second = block_scale(jax.random.fold_in(key, 22), expo)
    return (0.6 * turned + 0.8 * noise) * scale_second[None, :, None]


def setup_inputs(seed: int = 0) -> dict:
    key_of = jax.random.split(jax.random.key(seed), 5)
    first_state = draw_first_state(jax.random.fold_in(key_of[4], 71), 0)
    second_state = draw_second_state(jax.random.fold_in(key_of[4], 71), 0)
    place_first = draw_place_first(jax.random.fold_in(key_of[4], 71), 0)
    place_second = draw_place_second(jax.random.fold_in(key_of[4], 71), 0)
    return dict(first_state=first_state, second_state=second_state, place_first=place_first, place_second=place_second)


def reference(first_state, second_state, place_first, place_second):
    index_list = jnp.arange(BLOCKS, dtype=jnp.int32)
    logical_first = jnp.zeros((BLOCKS,), jnp.int32).at[place_first].set(index_list)
    source_blocks = place_second[logical_first].astype(jnp.int32)
    gathered = jnp.take(second_state, source_blocks, axis=1)
    amp_total = float(AMPS)
    first_sq = jnp.sum(lax.optimization_barrier(jnp.sum(first_state * first_state, axis=2)))
    second_sq = jnp.sum(lax.optimization_barrier(jnp.sum(second_state * second_state, axis=2)))
    real_sum = jnp.sum(lax.optimization_barrier(jnp.sum(first_state[0] * gathered[0] + first_state[1] * gathered[1], axis=1)))
    imag_sum = jnp.sum(lax.optimization_barrier(jnp.sum(first_state[0] * gathered[1] - first_state[1] * gathered[0], axis=1)))
    mean_first = first_sq / amp_total
    mean_second = second_sq / amp_total
    aligned = gathered / jnp.sqrt(mean_second + 1e-06)
    intersection = jnp.stack([real_sum, imag_sum]) / amp_total / jnp.sqrt((mean_first + 1e-06) * (mean_second + 1e-06))
    norms = jnp.stack([mean_first, mean_second])
    return (aligned, intersection, norms)
```

```python
import functools

import jax
import jax.numpy as jnp
from jax import lax
from jax.experimental import pallas as pl
from jax.experimental.pallas import tpu as pltpu
from jax.sharding import PartitionSpec as P

AXES = ("wide", "narrow")
LANES = 128
ANY = pl.BlockSpec(memory_space=pl.ANY)
SMEM = pl.BlockSpec(memory_space=pltpu.SMEM)
VMEM = pl.BlockSpec(memory_space=pltpu.VMEM)


def block_view(state):
    parts, blocks, block = state.shape
    tiles = state.reshape(parts, blocks // 8, 8, block // LANES, LANES)
    return tiles.transpose(0, 1, 3, 2, 4).reshape(parts, blocks // 8, block // LANES, 8, 1, LANES)


def block_array(view):
    parts, rows, cols = view.shape[:3]
    tiles = view.reshape(parts, rows, cols, 8, LANES).transpose(0, 1, 3, 2, 4)
    return tiles.reshape(parts, rows * 8, cols * LANES)


class Plan:
    def __init__(self, blocks_dev, block, devices):
        self.blocks_dev, self.block, self.devices = blocks_dev, block, devices
        self.share = blocks_dev // devices
        self.bits = (blocks_dev * devices).bit_length() - 1
        self.dev_bits = devices.bit_length() - 1
        self.free_bits = self.share.bit_length() - 1
        self.cols = block // LANES
        self.rows = 2 * self.share * self.cols
        self.send_free = 0
        self.recv_free = self.share
        self.send_dev = 2 * self.share
        self.recv_dev = self.send_dev + self.dev_bits
        self.table_size = -(-(self.recv_dev + self.dev_bits) // LANES) * LANES


def dev_offset(plan, table, base, device):
    total = jnp.int32(0)
    for j in range(plan.dev_bits):
        total += ((device >> j) & 1) * table[base + j]
    return total


def build_table(plan, first_rows, second_rows, table, send_bit, recv_bit):
    low = LANES.bit_length() - 1
    at_first, at_second = [], []
    for level in range(plan.bits):
        spot = (0, 0, 1 << level) if level < low else (level - low + 1, 0, 0)
        at_first.append(first_rows[spot])
        at_second.append(second_rows[spot])
    rank = jnp.int32(0)
    for one, two in zip(at_first, at_second):
        send_bit[rank] = two
        recv_bit[rank] = one
        rank += jnp.where((one < plan.blocks_dev) & (two < plan.blocks_dev), 1, 0)
    for j in range(plan.dev_bits):
        send, recv = jnp.int32(0), jnp.int32(0)
        for one, two in zip(at_first, at_second):
            send += jnp.where(one == plan.blocks_dev << j, two, 0)
            recv += jnp.where(two == plan.blocks_dev << j, one, 0)
        table[plan.send_dev + j] = send
        table[plan.recv_dev + j] = recv
    table[plan.send_free] = jnp.int32(0)
    table[plan.recv_free] = jnp.int32(0)
    for j in range(plan.free_bits):
        send, recv = send_bit[j], recv_bit[j]
        for low_part in range(1 << j):
            table[plan.send_free + (1 << j) + low_part] = table[plan.send_free + low_part] + send
            table[plan.recv_free + (1 << j) + low_part] = table[plan.recv_free + low_part] + recv


def start_rows(plan, table, free_base, offset, make):
    for part in range(2):
        def step(o, _):
            slot = offset + table[free_base + o]
            make(part, slot >> 3, slot & 7, (part * plan.share + o) * plan.cols).start()
            return 0
        lax.fori_loop(0, plan.share, step, 0, unroll=8)


def fill_messages(plan, table, dev_base, free_base, source, outs, buf, in_sems, out_sems, keys):
    me = lax.axis_index(AXES)
    n = plan.rows
    for j, key in enumerate(keys):
        offset = dev_offset(plan, table, dev_base, me ^ key)
        start_rows(plan, table, free_base, offset, lambda part, tile, sub, row: pltpu.make_async_copy(
            source.at[part, tile, :, sub], buf.at[pl.ds(j * n + row, plan.cols)], in_sems.at[j]))
    copies = []
    for j in range(len(keys)):
        piece = buf.at[pl.ds(j * n, n)]
        pltpu.make_async_copy(outs[j], piece, in_sems.at[j]).wait()
        copies.append(pltpu.make_async_copy(piece, outs[j], out_sems.at[j]))
        copies[-1].start()
    for copy in copies:
        copy.wait()


def message_scratch(plan, count):
    return [pltpu.VMEM((count * plan.rows, 1, LANES), jnp.float32),
            pltpu.SemaphoreType.DMA((count,)), pltpu.SemaphoreType.DMA((count,))]


def first_messages(plan, keys, second_view, first_place, second_place):
    count = len(keys)
    place_rows = plan.bits - (LANES.bit_length() - 1) + 1

    def body(second_ref, pf_ref, ps_ref, table, *rest):
        outs = rest[:count]
        first_rows, second_rows, send_bit, recv_bit, sem, buf, in_sems, out_sems = rest[count:]
        copies = []
        for j in range(place_rows):
            row = 0 if j == 0 else 1 << (j - 1)
            copies.append(pltpu.make_async_copy(pf_ref.at[row], first_rows.at[j], sem.at[2 * j]))
            copies.append(pltpu.make_async_copy(ps_ref.at[row], second_rows.at[j], sem.at[2 * j + 1]))
        for copy in copies:
            copy.start()
        for copy in copies:
            copy.wait()
        build_table(plan, first_rows, second_rows, table, send_bit, recv_bit)
        fill_messages(plan, table, plan.send_dev, plan.send_free, second_ref, outs, buf, in_sems, out_sems, keys)

    message = jax.ShapeDtypeStruct((plan.rows, 1, LANES), jnp.float32)
    return pl.pallas_call(
        body,
        name="first_messages",
        in_specs=[ANY, ANY, ANY],
        out_specs=[SMEM] + [ANY] * count,
        out_shape=[jax.ShapeDtypeStruct((plan.table_size,), jnp.int32)] + [message] * count,
        scratch_shapes=[pltpu.SMEM((place_rows, 1, LANES), jnp.int32), pltpu.SMEM((place_rows, 1, LANES), jnp.int32),
                        pltpu.SMEM((plan.bits + 1,), jnp.int32), pltpu.SMEM((plan.bits + 1,), jnp.int32),
                        pltpu.SemaphoreType.DMA((2 * place_rows,))] + message_scratch(plan, count),
        cost_estimate=pl.CostEstimate(flops=0, bytes_accessed=2 * count * plan.rows * LANES * 4, transcendentals=0),
    )(second_view, first_place.reshape(-1, 1, LANES), second_place.reshape(-1, 1, LANES))


def more_messages(plan, name, keys, dev_base, free_base, table, source_view):
    count = len(keys)

    def body(table_ref, source_ref, *rest):
        fill_messages(plan, table_ref, dev_base, free_base, source_ref, rest[:count], *rest[count:], keys)

    message = jax.ShapeDtypeStruct((plan.rows, 1, LANES), jnp.float32)
    return pl.pallas_call(
        body,
        name=name,
        in_specs=[SMEM, ANY],
        out_specs=[ANY] * count,
        out_shape=[message] * count,
        scratch_shapes=message_scratch(plan, count),
        cost_estimate=pl.CostEstimate(flops=0, bytes_accessed=2 * count * plan.rows * LANES * 4, transcendentals=0),
    )(table, source_view)


def take_messages(plan, name, keys, table, scale, firsts, messages, out_view, sums):
    count, n = len(keys), plan.rows
    fresh = isinstance(out_view, jax.ShapeDtypeStruct)

    def body(table_ref, scale_ref, *rest):
        first_refs, rest = rest[:count], rest[count:]
        message_refs, rest = rest[:count], rest[count:]
        if not fresh:
            sums_in, rest = rest[1], rest[2:]
        out_ref, sums_ref, first_buf, message_buf, placed, in_sems, out_sems = rest
        me = lax.axis_index(AXES)
        copies = []
        for j in range(count):
            piece = pl.ds(j * n, n)
            copies.append((pltpu.make_async_copy(first_refs[j], first_buf.at[piece], in_sems.at[2 * j]),
                           pltpu.make_async_copy(message_refs[j], message_buf.at[piece], in_sems.at[2 * j + 1])))
        for pair in copies:
            pair[0].start()
            pair[1].start()
        scale_value = scale_ref[0, 0]
        zero = jnp.zeros((8, LANES), jnp.float32)
        totals = (zero,) * 3 if fresh else tuple(sums_in[8 * i:8 * i + 8, :] for i in range(3))
        half = n // 2
        for j, key in enumerate(keys):
            copies[j][0].wait()
            copies[j][1].wait()

            def step(i, carry, j=j):
                real, imag, square = carry
                at = pl.multiple_of(j * n + i * 8, 8)
                at_imag = pl.multiple_of(j * n + half + i * 8, 8)
                f0, f1 = first_buf[pl.ds(at, 8), :], first_buf[pl.ds(at_imag, 8), :]
                g0, g1 = message_buf[pl.ds(at, 8), :], message_buf[pl.ds(at_imag, 8), :]
                placed[pl.ds(at, 8), 0, :] = g0 * scale_value
                placed[pl.ds(at_imag, 8), 0, :] = g1 * scale_value
                return (real + (f0 * g0 + f1 * g1), imag + (f0 * g1 - f1 * g0), square + (f0 * f0 + f1 * f1))

            totals = lax.fori_loop(0, half // 8, step, totals, unroll=8)
            offset = dev_offset(plan, table_ref, plan.recv_dev, me ^ key)
            start_rows(plan, table_ref, plan.recv_free, offset, lambda part, tile, sub, row: pltpu.make_async_copy(
                placed.at[pl.ds(j * n + row, plan.cols)], out_ref.at[part, tile, :, sub], out_sems.at[j]))
        for i in range(3):
            sums_ref[8 * i:8 * i + 8, :] = totals[i]
        for j in range(count):
            piece = placed.at[pl.ds(j * n, n)]
            pltpu.make_async_copy(piece, piece, out_sems.at[j]).wait()

    sums_shape = jax.ShapeDtypeStruct((24, LANES), jnp.float32)
    extra = () if fresh else (out_view, sums)
    alias = {} if fresh else {2 + 2 * count: 0}
    flat = [m.reshape(n, LANES) for m in (*firsts, *messages)]
    return pl.pallas_call(
        body,
        name=name,
        in_specs=[SMEM, SMEM] + [ANY] * (2 * count) + ([] if fresh else [ANY, VMEM]),
        out_specs=[ANY, VMEM],
        out_shape=[jax.ShapeDtypeStruct(out_view.shape, jnp.float32), sums_shape],
        scratch_shapes=[pltpu.VMEM((count * n, LANES), jnp.float32), pltpu.VMEM((count * n, LANES), jnp.float32),
                        pltpu.VMEM((count * n, 1, LANES), jnp.float32),
                        pltpu.SemaphoreType.DMA((2 * count,)), pltpu.SemaphoreType.DMA((count,))],
        input_output_aliases=alias,
        cost_estimate=pl.CostEstimate(flops=count * n * LANES * 8, bytes_accessed=3 * count * n * LANES * 4,
                                      transcendentals=0),
    )(table, scale, *flat, *extra)


def swap(value, key, devices):
    return lax.ppermute(value, AXES, [(d, d ^ key) for d in range(devices)])


def local(first_state, second_state, place_first, place_second):
    wide, narrow = lax.axis_size("wide"), lax.axis_size("narrow")
    devices = wide * narrow
    plan = Plan(first_state.shape[1], first_state.shape[2], devices)
    amp_total = float(first_state.shape[1] * devices * first_state.shape[2])
    half = narrow // 2
    others = range(1, devices)
    cross_head = [k for k in others if k % narrow == half]
    cross_head = cross_head[1:3] + cross_head[:1] + cross_head[3:]
    same = [k for k in others if k % narrow == 0]
    near = [k for k in others if 0 < k % narrow < half]
    cross_tail = [k for k in others if k % narrow > half]

    first_view, second_view = block_view(first_state), block_view(second_state)
    head = cross_head[:2]
    table, *built = first_messages(plan, head, second_view, place_first, place_second)
    outgoing = dict(zip(head, built))
    rest = cross_head[2:]
    outgoing.update(zip(rest, more_messages(plan, "messages_a", rest, plan.send_dev, plan.send_free, table, second_view)))
    rest = [0] + same + near + cross_tail
    outgoing.update(zip(rest, more_messages(plan, "messages_b", rest, plan.send_dev, plan.send_free, table, second_view)))
    every = [0] + cross_head + same + near + cross_tail
    firsts = dict(zip(every, more_messages(plan, "own_blocks", every, plan.recv_dev, plan.recv_free, table, first_view)))

    square = jnp.broadcast_to(jnp.sum(second_state * second_state), (1, LANES))
    for bit in range(wide.bit_length() - 1):
        square = square + swap(square, narrow << bit, devices)
    square = square + sum(swap(square, k, devices) for k in range(1, narrow))
    mean_second = square / amp_total
    scale = 1.0 / jnp.sqrt(mean_second + 1e-06)

    arrived = {0: outgoing[0]}
    for k in cross_head + same + near + cross_tail:
        arrived[k] = swap(outgoing[k], k, devices)

    tail = len(cross_tail)
    cuts = [tail // 2, tail * 3 // 4, tail - 1]
    groups = [[0] + cross_head, same + near]
    groups += [cross_tail[a:b] for a, b in zip([0] + cuts, cuts + [tail])]
    out_view, sums = jax.ShapeDtypeStruct(first_view.shape, jnp.float32), None
    for i, keys in enumerate(groups):
        out_view, sums = take_messages(plan, f"take_{i}", keys, table, scale, [firsts[k] for k in keys],
                                       [arrived[k] for k in keys], out_view, sums)
    for bit in range(devices.bit_length() - 1):
        sums = sums + swap(sums, 1 << bit, devices)
    real, imag, first_sq = jnp.sum(sums.reshape(3, -1), axis=1)
    mean_first = first_sq / amp_total
    mean_second = mean_second[0, 0]
    intersection = (jnp.stack([real, imag]) / amp_total
                    / jnp.sqrt((mean_first + 1e-06) * (mean_second + 1e-06)))
    return block_array(out_view), intersection, jnp.stack([mean_first, mean_second])


def solution(mesh):
    return jax.shard_map(
        local,
        mesh=mesh,
        in_specs=(P(None, AXES, None), P(None, AXES, None), P(), P()),
        out_specs=(P(None, AXES, None), P(), P()),
        check_vma=False,
    )
```
